32 devices in a mesh: dp: 4 (over y, x), ctx: 8 (over z, core).
Axes of the slice: x: 2, y: 2, z: 4, core: 2. Of those that a mesh axis runs over, the one named last changes fastest.
Arguments:
- query_rows: bfloat16 [4096, 2048], P(('dp', 'ctx')), may hold values from -64 to 64
- key_rows: bfloat16 [4096, 2048], P(('dp', 'ctx')), may hold values from -64 to 64
- value_rows: bfloat16 [4096, 2048], P(('dp', 'ctx')), may hold values from -6 to 6
- cotangent: bfloat16 [4096, 2048], P(('dp', 'ctx')), may hold values from -6 to 6
- query_gain: float32 [2048], replicated, may hold values from 0.5 to 5.5
- key_gain: float32 [2048], replicated, may hold values from 0.5 to 5.5
- positions: int32 [4096], P(('dp', 'ctx')), may hold values from 0 to 511, as said below
- span_start: int32 [8, 2], P('dp'), may hold values from 0 to 384, as said below
- span_length: int32 [8, 2], P('dp'), may hold values from 64 to 128
Outputs:
- output: bfloat16 [4096, 2048], P(('dp', 'ctx'))
- query_grad: bfloat16 [4096, 2048], P(('dp', 'ctx'))
- key_grad: bfloat16 [4096, 2048], P(('dp', 'ctx'))
- value_grad: bfloat16 [4096, 2048], P(('dp', 'ctx'))
- gain_grads: float32 [2, 2048], replicated
The draws below stay inside these ranges and needn't reach their ends.
Inputs may be any that keep to these rules, and one draw needn't show every extreme that they name: Within each sequence every position 0 to 511 appears once; each block's rows are two runs of 64 consecutive positions, each run in increasing order. `span_start`: the first span of a sequence starts at 128 or earlier, the second at 256 or later; spans don't intersect and end inside the sequence.
All inputs are finite; a program needn't handle non-finite values.
Results may differ from the reference program's by a relative error of at most 0.035.
The reference program's roundings to bfloat16 on the way count: a program that leaves them out, or rounds other values in their place, can miss the bound.
Values may be sent and summed in bfloat16 or wider, within the bound.
No kernel may reach another device: no remote copies, remote signals or barrier semaphores. Data moves between devices by JAX's collectives and lax.ppermute only.
A program may use at most 128 MiB of HBM per device.

```python
import jax
import jax.numpy as jnp
from jax import lax

HEADS = 16
HEAD = 128
TOK_DEV = 128
SEQS_CTX = 2
NSPAN = 2
CYCLE = 4
LEN = 512
SPAN = 128
PIECE = 64
NSEQ = 8
ROWS = 4096
N_DP = 4


def query_base(key):
    sample_draw = jax.random.normal(jax.random.fold_in(key, 101), (ROWS, HEADS * HEAD), jnp.float32)
    return jnp.clip(sample_draw, -64.0, 64.0)


def draw_query_rows(key, part):
    return query_base(key).astype(jnp.bfloat16)


def draw_key_rows(key, part):
    fresh_keys = jax.random.normal(jax.random.fold_in(key, 201), (ROWS, HEADS * HEAD), jnp.float32)
    return jnp.clip(fresh_keys, -64.0, 64.0).astype(jnp.bfloat16)


def gain_draw(key, salt_id):
    channel = jax.random.uniform(jax.random.fold_in(key, salt_id), (HEADS, HEAD), jnp.float32, 0.6, 1.6)
    return channel.reshape(HEADS * HEAD).astype(jnp.float32)


def draw_query_gain(key, part):
    return gain_draw(key, 302)


def draw_key_gain(key, part):
    return gain_draw(key, 303)


def draw_positions(key, part):
    seq_keys = jax.random.split(jax.random.fold_in(key, 501), NSEQ)
    orders = jax.vmap(lambda single: jax.random.permutation(single, 2 * CYCLE))(seq_keys)
    orders = orders.reshape(N_DP, SEQS_CTX, CYCLE, 2)
    orders = jnp.transpose(orders, (0, 2, 1, 3))
    places = orders[..., None] * PIECE + jnp.arange(PIECE, dtype=jnp.int32)
    return places.reshape(ROWS).astype(jnp.int32)


def draw_span_start(key, part):
    first_start = jax.random.randint(jax.random.fold_in(key, 401), (NSEQ,), 0, LEN // 2 - SPAN + 1)
    second = jax.random.randint(jax.random.fold_in(key, 402), (NSEQ,), LEN // 2, LEN - SPAN + 1)
    return jnp.stack([first_start, second], axis=1).astype(jnp.int32)


def set_ends(result, rng, smallest, largest):
    extent = result.shape
    place = [jax.random.randint(jax.random.fold_in(rng, axis), (), 0, extent[axis]) for axis in range(len(extent))]
    result = result.at[tuple(place)].set(smallest)
    longest = extent.index(max(extent))
    place[longest] = (place[longest] + 1) % extent[longest]
    return result.at[tuple(place)].set(largest)


def shard_levels(key, extent, pieces, least, largest):
    factor_of, own = 1.0, jax.random.fold_in(key, 6)
    for position, shards_of in pieces:
        draws = jnp.exp(jax.random.uniform(jax.random.fold_in(own, position), (shards_of,), jnp.float32, least / len(pieces), largest / len(pieces)))
        factor_of = factor_of * jnp.repeat(draws, extent[position] // shards_of).reshape([-1 if axis == position else 1 for axis in range(len(extent))])
    return factor_of


def scatter_about(key, extent, spread, most, pieces=(), kind=jnp.bfloat16):
    array = jax.random.normal(key, extent, jnp.float32) * spread
    if len(pieces) > 0:
        array = shard_levels(key, extent, pieces, -0.22, 0.18) * array
    return jnp.clip(array, min=-most, max=most).astype(kind)


def setup_inputs(seed: int = 0) -> dict:
    splits = jax.random.split(jax.random.key(seed), 10)
    return {
        "query_rows": draw_query_rows(jax.random.fold_in(splits[9], 71), 0),
        "key_rows": draw_key_rows(jax.random.fold_in(splits[9], 71), 0),
        "value_rows": scatter_about(splits[2], (ROWS, HEADS * HEAD), 1.0, 6.0, ((0, 32),)),
        "cotangent": scatter_about(splits[3], (ROWS, HEADS * HEAD), 1.0, 6.0, ((0, 32),)),
        "query_gain": draw_query_gain(jax.random.fold_in(splits[9], 71), 0),
        "key_gain": draw_key_gain(jax.random.fold_in(splits[9], 71), 0),
        "positions": draw_positions(jax.random.fold_in(splits[9], 71), 0),
        "span_start": draw_span_start(jax.random.fold_in(splits[9], 71), 0),
        "span_length": set_ends(jax.random.randint(splits[8], (NSEQ, NSPAN), SPAN // 2, SPAN + 1), jax.random.fold_in(splits[8], 1), SPAN // 2, SPAN).astype(jnp.int32),
    }


epsilon = 1e-05
masked_score = -1e+30

def normalize(raw_rows, gain_row):
    values = raw_rows.astype(jnp.float32).reshape(raw_rows.shape[0], HEADS, HEAD)
    inverse = lax.rsqrt(lax.optimization_barrier(jnp.mean(values * values, axis=-1, keepdims=True)) + epsilon)
    unit_rows = values * inverse
    return (unit_rows, inverse, (unit_rows * gain_row.reshape(HEADS, HEAD)).astype(jnp.bfloat16))

def norm_backward(grad_normed, unit_rows, inverse, gain_row):
    grad_unit = grad_normed * gain_row.reshape(HEADS, HEAD)
    projected = lax.optimization_barrier(jnp.mean(grad_unit * unit_rows, axis=-1, keepdims=True))
    grad_raw = inverse * (grad_unit - unit_rows * projected)
    gain_part = lax.optimization_barrier(jnp.sum(grad_normed * unit_rows, axis=0)).reshape(HEADS * HEAD)
    return (grad_raw.reshape(grad_raw.shape[0], HEADS * HEAD).astype(jnp.bfloat16), gain_part)

def span_labels(places, starts, lengths):
    inside = (places[:, None] >= starts[None, :]) & (places[:, None] < starts[None, :] + lengths[None, :])
    span_ids = jnp.arange(1, starts.shape[0] + 1, dtype=jnp.int32)
    return lax.optimization_barrier(jnp.sum(jnp.where(inside, span_ids[None, :], 0), axis=1)).astype(jnp.int32)

def visible(query_places, query_labels, key_places, key_labels):
    causal = key_places[None, :] <= query_places[:, None]
    same_span = (query_labels[:, None] == key_labels[None, :]) & (query_labels[:, None] > 0)
    return causal | same_span

def to_sequences(tensor):
    trailing = tensor.shape[1:]
    shaped = tensor.reshape((N_DP, CYCLE, SEQS_CTX, TOK_DEV) + trailing)
    return jnp.swapaxes(shaped, 1, 2).reshape((NSEQ, LEN) + trailing)

def from_sequences(tensor):
    trailing = tensor.shape[2:]
    shaped = tensor.reshape((N_DP, SEQS_CTX, CYCLE, TOK_DEV) + trailing)
    return jnp.swapaxes(shaped, 1, 2).reshape((ROWS,) + trailing)

def rounded(tensor):
    return lax.optimization_barrier(tensor.astype(jnp.bfloat16)).astype(jnp.float32)

def one_sequence(packed):
    query_normed, key_normed, value_block, out_grads, places, starts, lengths = packed
    score_scale = HEAD ** (-0.5)
    labels = span_labels(places, starts, lengths)
    allowed = visible(places, labels, places, labels)

    def one_head(head_pack):
        query_float, key_float, value_float, grad_float = head_pack
        scores = jnp.einsum('qd,kd->qk', query_float, key_float) * score_scale
        scores = jnp.where(allowed, scores, masked_score)
        row_max = lax.optimization_barrier(jnp.max(scores, axis=-1, keepdims=True))
        log_total = row_max + jnp.log(lax.optimization_barrier(jnp.sum(jnp.exp(scores - row_max), axis=-1, keepdims=True)))
        attn_probs = jnp.exp(scores - log_total)
        weights = rounded(attn_probs)
        output = jnp.einsum('qk,kd->qd', weights, value_float)
        row_delta = lax.optimization_barrier(jnp.sum(rounded(output) * grad_float, axis=-1, keepdims=True))
        grad_values = jnp.einsum('qk,qd->kd', weights, grad_float).astype(jnp.bfloat16)
        prob_grads = jnp.einsum('qd,kd->qk', grad_float, value_float)
        score_grads = rounded(attn_probs * (prob_grads - row_delta))
        grad_query = jnp.einsum('qk,kd->qd', score_grads, key_float) * score_scale
        grad_keys = jnp.einsum('qk,qd->kd', score_grads, query_float) * score_scale
        return (output.astype(jnp.bfloat16), grad_values, grad_query, grad_keys)
    head_major = tuple((jnp.transpose(tensor.astype(jnp.float32), (1, 0, 2)) for tensor in (query_normed, key_normed, value_block, out_grads)))
    results = lax.map(one_head, head_major)
    return tuple((jnp.transpose(tensor, (1, 0, 2)) for tensor in results))

def reference(query_rows, key_rows, value_rows, cotangent, query_gain, key_gain, positions, span_start, span_length):
    query_unit, query_inverse, query_normed = normalize(query_rows, query_gain)
    key_unit, key_inverse, key_normed = normalize(key_rows, key_gain)
    packed = (to_sequences(query_normed), to_sequences(key_normed), to_sequences(value_rows.reshape(ROWS, HEADS, HEAD)), to_sequences(cotangent.reshape(ROWS, HEADS, HEAD)), to_sequences(positions), span_start, span_length)
    output, grad_values, grad_query, grad_keys = lax.map(one_sequence, packed)
    output = from_sequences(output).reshape(ROWS, HEADS * HEAD)
    value_grad = from_sequences(grad_values).reshape(ROWS, HEADS * HEAD)
    query_grad, query_part = norm_backward(from_sequences(grad_query), query_unit, query_inverse, query_gain)
    key_grad, key_part = norm_backward(from_sequences(grad_keys), key_unit, key_inverse, key_gain)
    gain_grads = jnp.stack([query_part, key_part])
    return (output, query_grad, key_grad, value_grad, gain_grads)
```

```python
import functools

import jax
import jax.numpy as jnp
from jax import lax
from jax.experimental import pallas as pl
from jax.experimental.pallas import tpu as pltpu
from jax.sharding import PartitionSpec as P

HEADS = 16
HEAD = 128
SEQS_CTX = 2
TENSORS = 4
TAIL = 16
RADIX = 256

epsilon = 1e-05
masked_score = -1e30


VMEM = pltpu.VMEM
SMEM = pltpu.SMEM
ANY = pl.ANY


def spec(space):
    return pl.BlockSpec(memory_space=space)


def pack_kernel(members, per_device, width, offset, tail, *refs):
    me_ref, places_ref = refs[0], refs[1]
    sources = refs[2 : 2 + TENSORS]
    outs = refs[2 + TENSORS : 2 + TENSORS + members]
    sems = refs[-1]
    me = me_ref[0]
    rows = sources[0].shape[0]
    copies = []
    for step in range(members):
        shift = (step + 1) % members
        owner = lax.rem(me + shift, members)
        start = pl.multiple_of(owner * (per_device * HEAD) + offset, HEAD)
        for t in range(TENSORS):
            copy = pltpu.make_async_copy(
                sources[t].at[:, pl.ds(start, width)],
                outs[shift].at[pl.ds(t * rows, rows), :],
                sems.at[shift, t],
            )
            copy.start()
            copies.append(copy)
    if tail:
        places = places_ref[...]
        high = (places // RADIX).astype(jnp.float32)
        low = (places % RADIX).astype(jnp.float32)
        half = TAIL // 2
        block = jnp.concatenate(
            [jnp.broadcast_to(high, (half, rows)), jnp.broadcast_to(low, (half, rows))], axis=0
        ).astype(jnp.bfloat16)
        for shift in range(members):
            outs[shift][TENSORS * rows : TENSORS * rows + TAIL, :HEAD] = block
            if width > HEAD:
                outs[shift][TENSORS * rows : TENSORS * rows + TAIL, HEAD:] = jnp.zeros(
                    (TAIL, width - HEAD), jnp.bfloat16
                )
    for copy in copies:
        copy.wait()


def pack(me, places, arrays, members, per_device, width, offset, tail):
    rows = arrays[0].shape[0]
    total = TENSORS * rows + (TAIL if tail else 0)
    return pl.pallas_call(
        functools.partial(pack_kernel, members, per_device, width, offset, tail),
        out_shape=[jax.ShapeDtypeStruct((total, width), jnp.bfloat16)] * members,
        in_specs=[spec(SMEM), spec(VMEM)] + [spec(ANY)] * TENSORS,
        out_specs=[spec(VMEM)] * members,
        scratch_shapes=[pltpu.SemaphoreType.DMA((members, TENSORS))],
        name="pack",
    )(me, places, *arrays)


def normalize(raw):
    values = raw.astype(jnp.float32)
    inverse = lax.rsqrt(jnp.mean(values * values, axis=-1, keepdims=True) + epsilon)
    return values * inverse, inverse


def norm_backward(grad_normed, unit, inverse, gain):
    grad_unit = grad_normed * gain
    projected = jnp.mean(grad_unit * unit, axis=-1, keepdims=True)
    return (inverse * (grad_unit - unit * projected)).astype(jnp.bfloat16)


def dot(a, b, contract):
    return lax.dot_general(a, b, ((contract[:1], contract[1:]), ((), ())), preferred_element_type=jnp.float32)


def label_of(places, spans_ref, seq):
    label = jnp.zeros_like(places)
    for s in range(spans_ref.shape[2]):
        start = spans_ref[0, seq, s]
        stop = start + spans_ref[1, seq, s]
        inside = (places >= start) & (places < stop)
        label = label + jnp.where(inside, s + 1, 0)
    return label


def attention_kernel(members, heads, offset, per_device, first, *refs):
    rows = HEAD
    where_ref, spans_ref, gains_ref, places_in = refs[0], refs[1], refs[2], refs[3]
    packs = refs[4 : 4 + members]
    outs = refs[4 + members : 4 + 2 * members]
    gain_out, places_out = refs[4 + 2 * members], refs[5 + 2 * members]
    keys, dkeys, dvalues, values = refs[6 + 2 * members :]
    me, seq = where_ref[0], where_ref[1]
    scale = HEAD ** (-0.5)
    length = members * rows

    if first:
        half = TAIL // 2
        for m in range(members):
            tail = packs[m][TENSORS * rows : TENSORS * rows + TAIL, :HEAD].astype(jnp.float32)
            places_out[m] = (tail[:half] * RADIX + tail[half:]).astype(jnp.int32)
        places_of = places_out
    else:
        places_out[...] = places_in[...]
        places_of = places_in

    key_places = jnp.concatenate([places_of[m][:1] for m in range(members)], axis=1)
    key_labels = label_of(key_places, spans_ref, seq)

    start = pl.multiple_of(me * (per_device * HEAD) + offset, HEAD)
    gain_rows = gains_ref[:, pl.ds(start, heads * HEAD)]

    def tensor(m, t, h):
        return packs[m][t * rows : (t + 1) * rows, h * HEAD : (h + 1) * HEAD]

    for h in range(heads):
        lanes = slice(h * HEAD, (h + 1) * HEAD)
        key_gain = gain_rows[1:2, lanes]
        for m in range(members):
            unit, _ = normalize(tensor(m, 1, h))
            keys[h, m * rows : (m + 1) * rows, :] = (unit * key_gain).astype(jnp.bfloat16)
            values[h, m * rows : (m + 1) * rows, :] = tensor(m, 2, h)
    gain_sums = [[None, None] for _ in range(heads)]
    for m in range(members):
        wide = jnp.broadcast_to(places_of[m][:1].astype(jnp.float32), (rows, rows))
        query_places = jnp.transpose(wide)[:, :1].astype(jnp.int32)
        query_labels = label_of(query_places, spans_ref, seq)
        allowed = (key_places <= query_places) | (
            (key_labels == query_labels) & (query_labels > 0)
        )
        for h in range(heads):
            lanes = slice(h * HEAD, (h + 1) * HEAD)
            query_gain = gain_rows[0:1, lanes]
            unit, inverse = normalize(tensor(m, 0, h))
            query = (unit * query_gain).astype(jnp.bfloat16)
            grads = tensor(m, 3, h)
            key_all = keys[h]
            value_all = values[h]
            scores = jnp.where(allowed, dot(query, key_all, (1, 1)) * scale, masked_score)
            top = jnp.max(scores, axis=-1, keepdims=True)
            exps = jnp.exp(scores - top)
            probs = exps * (1.0 / jnp.sum(exps, axis=-1, keepdims=True))
            weights = probs.astype(jnp.bfloat16)
            output = dot(weights, value_all, (1, 0)).astype(jnp.bfloat16)
            outs[m][0:rows, lanes] = output
            delta = jnp.sum(
                output.astype(jnp.float32) * grads.astype(jnp.float32), axis=-1, keepdims=True
            )
            dvalue = dot(weights, grads, (0, 0))
            prob_grads = dot(grads, value_all, (1, 1))
            score_grads = (probs * (prob_grads - delta)).astype(jnp.bfloat16)
            dquery = dot(score_grads, key_all, (1, 0)) * scale
            dkey = dot(score_grads, query, (0, 0))
            if m == 0:
                dvalues[h] = dvalue
                dkeys[h] = dkey
            else:
                dvalues[h] += dvalue
                dkeys[h] += dkey
            outs[m][rows : 2 * rows, lanes] = norm_backward(dquery, unit, inverse, query_gain)
            part = jnp.sum(dquery * unit, axis=0, keepdims=True)
            gain_sums[h][0] = part if m == 0 else gain_sums[h][0] + part
    for h in range(heads):
        lanes = slice(h * HEAD, (h + 1) * HEAD)
        key_gain = gain_rows[1:2, lanes]
        for m in range(members):
            block = slice(m * rows, (m + 1) * rows)
            unit, inverse = normalize(tensor(m, 1, h))
            dkey = dkeys[h, block, :] * scale
            outs[m][2 * rows : 3 * rows, lanes] = norm_backward(dkey, unit, inverse, key_gain)
            part = jnp.sum(dkey * unit, axis=0, keepdims=True)
            gain_sums[h][1] = part if m == 0 else gain_sums[h][1] + part
            outs[m][3 * rows : 4 * rows, lanes] = dvalues[h, block, :].astype(jnp.bfloat16)
        gain_out[0:1, lanes] = gain_sums[h][0]
        gain_out[1:2, lanes] = gain_sums[h][1]


def attention(where, spans, gains, places, packs, members, heads, offset, per_device, first):
    rows = HEAD
    length = members * rows
    width = heads * HEAD
    flops = heads * 6 * 2 * length * length * HEAD
    result = pl.pallas_call(
        functools.partial(attention_kernel, members, heads, offset, per_device, first),
        out_shape=[jax.ShapeDtypeStruct((TENSORS * rows, width), jnp.bfloat16)] * members
        + [
            jax.ShapeDtypeStruct((2, width), jnp.float32),
            jax.ShapeDtypeStruct((members, TAIL // 2, rows), jnp.int32),
        ],
        in_specs=[spec(SMEM), spec(SMEM)] + [spec(VMEM)] * (2 + members),
        out_specs=[spec(VMEM)] * (members + 2),
        scratch_shapes=[
            VMEM((heads, length, HEAD), jnp.bfloat16),
            VMEM((heads, length, HEAD), jnp.float32),
            VMEM((heads, length, HEAD), jnp.float32),
            VMEM((heads, length, HEAD), jnp.bfloat16),
        ],
        cost_estimate=pl.CostEstimate(
            flops=flops,
            bytes_accessed=2 * TENSORS * length * width * 2,
            transcendentals=heads * length * length,
        ),
        name="attention",
    )(where, spans, gains, places, *packs)
    return result[:members], result[members], result[members + 1]


def unpack_kernel(members, per_device, width, offset, final, *refs):
    me_ref = refs[0]
    packs = refs[1 : 1 + members]
    at = 1 + members
    if final:
        gains = refs[at : at + members]
        at += members + TENSORS
    outs = refs[at : at + TENSORS]
    sems = refs[-1]
    me = me_ref[0]
    rows = outs[0].shape[0]
    copies = []
    for shift in range(members):
        owner = lax.rem(me + shift, members)
        start = pl.multiple_of(owner * (per_device * HEAD) + offset, HEAD)
        for t in range(TENSORS):
            copy = pltpu.make_async_copy(
                packs[shift].at[pl.ds(t * rows, rows), :],
                outs[t].at[:, pl.ds(start, width)],
                sems.at[shift, t],
            )
            copy.start()
            copies.append(copy)
    if final:
        gain_out = refs[at + TENSORS]
        for shift in range(members):
            owner = lax.rem(me + members - shift, members)
            start = pl.multiple_of(owner * (per_device * HEAD), HEAD)
            gain_out[:, pl.ds(start, per_device * HEAD)] = gains[shift][...]
    for copy in copies:
        copy.wait()


def unpack(me, packs, members, per_device, width, offset, gains=None, into=None):
    rows = packs[0].shape[0] // TENSORS
    final = gains is not None
    shape = jax.ShapeDtypeStruct((rows, HEADS * HEAD), jnp.bfloat16)
    out_shape = [shape] * TENSORS
    in_specs = [spec(SMEM)] + [spec(VMEM)] * members
    out_specs = [spec(ANY)] * TENSORS
    operands = [me, *packs]
    aliases = {}
    if final:
        operands += list(gains)
        in_specs += [spec(VMEM)] * members
        if into is None:
            into = [jnp.zeros(shape.shape, shape.dtype) for _ in range(TENSORS)]
        aliases = {len(operands) + t: t for t in range(TENSORS)}
        operands += list(into)
        in_specs += [spec(ANY)] * TENSORS
        out_shape = out_shape + [jax.ShapeDtypeStruct((2, HEADS * HEAD), jnp.float32)]
        out_specs = out_specs + [spec(VMEM)]
    return pl.pallas_call(
        functools.partial(unpack_kernel, members, per_device, width, offset, final),
        out_shape=out_shape,
        in_specs=in_specs,
        out_specs=out_specs,
        scratch_shapes=[pltpu.SemaphoreType.DMA((members, TENSORS))],
        input_output_aliases=aliases,
        name="unpack",
    )(*operands)


def body(
    query_rows,
    key_rows,
    value_rows,
    cotangent,
    query_gain,
    key_gain,
    positions,
    span_start,
    span_length,
):
    axis_count = lax.axis_size("ctx")
    dp_count = lax.axis_size("dp")
    members = axis_count // SEQS_CTX
    per_device = HEADS // members
    chunks = 2 if per_device % 2 == 0 else 1
    heads = per_device // chunks
    width = heads * HEAD
    ctx_index = lax.axis_index("ctx")
    member = (ctx_index // SEQS_CTX).astype(jnp.int32)
    seq = (ctx_index % SEQS_CTX).astype(jnp.int32)
    me = member.reshape(1)
    where = jnp.stack([member, seq])
    spans = jnp.stack([span_start, span_length])
    gains = jnp.stack([query_gain, key_gain])
    places = positions.reshape(1, -1)

    def along(tensor, shift):
        pairs = [(i, (i + SEQS_CTX * shift) % axis_count) for i in range(axis_count)]
        return lax.ppermute(tensor, "ctx", pairs)

    arrays = (query_rows, key_rows, value_rows, cotangent)
    received = []
    for c in range(chunks):
        sends = pack(me, places, arrays, members, per_device, width, c * width, c == 0)
        received.append([sends[0]] + [along(sends[s], s) for s in range(1, members)])
    returned, gain_parts = [], []
    all_places = jnp.zeros((members, TAIL // 2, HEAD), jnp.int32)
    for c in range(chunks):
        outs, part, all_places = attention(
            where, spans, gains, all_places, received[c], members, heads, c * width, per_device, c == 0
        )
        gain_parts.append(part)
        returned.append([outs[0]] + [along(outs[s], -s) for s in range(1, members)])
    total = jnp.concatenate(gain_parts, axis=1)
    total = total + lax.ppermute(total, "ctx", [(i, i ^ 1) for i in range(axis_count)])
    bit = 1
    while bit < dp_count:
        total = total + lax.ppermute(total, "dp", [(i, i ^ bit) for i in range(dp_count)])
        bit *= 2
    gain_all = [total] + [along(total, s) for s in range(1, members)]
    into = None
    for c in range(chunks):
        final = c == chunks - 1
        into = unpack(
            me, returned[c], members, per_device, width, c * width, gain_all if final else None, into
        )
    output, query_grad, key_grad, value_grad, gain_grads = into
    return output, query_grad, key_grad, value_grad, gain_grads


def solution(mesh):
    rows = P(("dp", "ctx"), None)
    in_specs = (rows, rows, rows, rows, P(), P(), P(("dp", "ctx")), P("dp", None), P("dp", None))
    out_specs = (rows, rows, rows, rows, P())
    return jax.shard_map(body, mesh=mesh, in_specs=in_specs, out_specs=out_specs, check_vma=False)
```
